32 devices in a mesh: sp: 4 (over x, core), tp: 8 (over z, y).
Axes of the slice: x: 2, y: 2, z: 4, core: 2. Of those that a mesh axis runs over, the one named last changes fastest.
Arguments:
- tokens: bfloat16 [8, 220, 4096], P(None, 'sp'), may hold values from -6 to 6
- modulation: float32 [6, 4096], replicated, may hold values from -2.5 to 2.5
- w_qkv: bfloat16 [4096, 3, 4096], P('sp', None, 'tp'), may hold values from -4 to 4
- w_out: bfloat16 [4096, 4096], P('tp', 'sp'), may hold values from -0.09375 to 0.09375
- w_up: bfloat16 [4096, 16384], P('sp', 'tp'), may hold values from -0.09375 to 0.09375
- w_down: bfloat16 [16384, 4096], P('tp', 'sp'), may hold values from -0.046875 to 0.046875
Outputs:
- block_out: bfloat16 [8, 220, 4096], P(None, 'sp', 'tp')
The draws below stay inside these ranges and needn't reach their ends.
All inputs are finite; a program needn't handle non-finite values.
Results may differ from the reference program's by a relative error of at most 0.012.
Values may be sent and summed in bfloat16 or wider, within the bound.
A program may use at most 128 MiB of HBM per device.

```python
import jax
import jax.numpy as jnp
from jax import lax

D = 4096
HEADS = 32
DH = 128
FF = 16384
FRAMES = 8
PATCHES = 220
N_TP = 8


def draw_w_qkv(key, part):
    inner = HEADS * DH
    base = jax.random.normal(key, (D, 3, inner), jnp.float32) * D ** (-0.5)
    factor = jnp.array([1.3, 1.3, 1.0], jnp.float32)
    base = base * factor[None, :, None]
    base = jnp.clip(base, -4.0, 4.0)
    return base.astype(jnp.bfloat16)


def block_scale(rng, shape, pieces, low, top_value):
    loudness = 1.0
    for axis_at, shards_of in pieces:
        steps = jax.random.uniform(jax.random.fold_in(jax.random.fold_in(rng, 6), axis_at), (shards_of,), jnp.float32, low / len(pieces), top_value / len(pieces))
        loudness = loudness * jnp.repeat(jnp.exp(steps), shape[axis_at] // shards_of).reshape((-1,) + (1,) * (len(shape) - 1 - axis_at))
    return loudness


def normal_values(stream_key, extent, scale, bound, cuts=(), held_as=jnp.bfloat16):
    level = block_scale(stream_key, extent, cuts, -0.22, 0.18) if cuts else 1.0
    drawn = jax.random.normal(stream_key, extent, jnp.float32) * scale * level
    return jnp.minimum(jnp.maximum(drawn, -bound), bound).astype(held_as)


def setup_inputs(seed: int = 0) -> dict:
    keys = jax.random.split(jax.random.key(seed), 7)
    tokens = normal_values(keys[0], (FRAMES, PATCHES, D), 1.0, 6.0, ((1, 4),))
    modulation = normal_values(keys[1], (6, D), 0.5, 2.5, (), jnp.float32)
    w_qkv = draw_w_qkv(jax.random.fold_in(keys[6], 71), 0)
    w_out = normal_values(keys[3], (HEADS * DH, D), (HEADS * DH) ** -0.5, 0.09375, ((0, 8), (1, 4)))
    w_up = normal_values(keys[4], (D, FF), D ** -0.5, 0.09375, ((0, 4), (1, 8)))
    w_down = normal_values(keys[5], (FF, D), FF ** -0.5, 0.046875, ((0, 8), (1, 4)))
    return {"tokens": tokens, "modulation": modulation, "w_qkv": w_qkv, "w_out": w_out, "w_up": w_up, "w_down": w_down}


EPSILON = 1e-06

def normalize(tok_rows, shift_vec, scale_vec):
    values = tok_rows.astype(jnp.float32)
    center = lax.optimization_barrier(jnp.mean(values, axis=-1, keepdims=True))
    spread = lax.optimization_barrier(jnp.mean(jnp.square(values - center), axis=-1, keepdims=True))
    scaled = (values - center) * lax.rsqrt(spread + EPSILON)
    return (scaled * (1.0 + scale_vec) + shift_vec).astype(jnp.bfloat16)

def attend_single(triple):
    query_rows, key_rows, value_rows = triple
    factor = query_rows.shape[-1] ** (-0.5)
    scores = lax.dot_general(query_rows, key_rows, (((1,), (1,)), ((), ())), preferred_element_type=jnp.float32) * factor
    row_max = lax.optimization_barrier(jnp.max(scores, axis=1, keepdims=True))
    raw_weights = jnp.exp(scores - row_max)
    att_weights = (raw_weights / lax.optimization_barrier(jnp.sum(raw_weights, axis=1, keepdims=True))).astype(jnp.bfloat16)
    return jnp.dot(att_weights, value_rows, preferred_element_type=jnp.float32).astype(jnp.bfloat16)

def reference(tokens, modulation, w_qkv, w_out, w_up, w_down):
    frames, patches, width = tokens.shape
    heads_local = HEADS // N_TP
    inner = heads_local * DH
    hidden_local = FF // N_TP
    mod_a = normalize(tokens, modulation[0], modulation[1]).reshape(frames * patches, width)

    def attn_group(group, running):
        begin = (group * inner).astype(jnp.int32)
        weight_group = lax.dynamic_slice_in_dim(w_qkv, begin, inner, 2).reshape(width, 3 * inner)
        projected = jnp.dot(mod_a, weight_group, preferred_element_type=jnp.float32).astype(jnp.bfloat16)
        projected = projected.reshape(frames, patches, 3, heads_local, DH)
        stacked = jnp.transpose(projected, (2, 0, 3, 1, 4)).reshape(3, frames * heads_local, patches, DH)
        attended = lax.map(attend_single, (stacked[0], stacked[1], stacked[2]))
        attended = attended.reshape(frames, heads_local, patches, DH)
        rows_group = lax.dynamic_slice_in_dim(w_out, begin, inner, 0).reshape(heads_local, DH, width)
        term = jnp.einsum('fhpd,hde->fpe', attended.astype(jnp.float32), rows_group.astype(jnp.float32))
        term = lax.optimization_barrier(term.astype(jnp.bfloat16)).astype(jnp.float32)
        return running + term
    attn_sum = lax.fori_loop(0, N_TP, attn_group, jnp.zeros((frames, patches, width), jnp.float32))
    middle = (tokens.astype(jnp.float32) + modulation[2] * attn_sum).astype(jnp.bfloat16)
    mod_b = normalize(middle, modulation[3], modulation[4]).reshape(frames * patches, width)

    def mlp_group(group, running):
        begin = (group * hidden_local).astype(jnp.int32)
        up_cols = lax.dynamic_slice_in_dim(w_up, begin, hidden_local, 1)
        hidden = jax.nn.gelu(jnp.dot(mod_b, up_cols, preferred_element_type=jnp.float32), approximate=True).astype(jnp.bfloat16)
        down_rows = lax.dynamic_slice_in_dim(w_down, begin, hidden_local, 0)
        term = jnp.dot(hidden, down_rows, preferred_element_type=jnp.float32)
        term = lax.optimization_barrier(term.astype(jnp.bfloat16)).astype(jnp.float32)
        return running + term.reshape(frames, patches, width)
    mlp_sum = lax.fori_loop(0, N_TP, mlp_group, jnp.zeros((frames, patches, width), jnp.float32))
    return (middle.astype(jnp.float32) + modulation[5] * mlp_sum).astype(jnp.bfloat16)
```

```python
import math

import jax
import jax.numpy as jnp
from jax import lax
from jax.sharding import PartitionSpec as P

DH = 128
EPSILON = 1e-06
MLP_CHUNKS = 4
BF = jnp.bfloat16
F32 = jnp.float32


def normalize(tok_rows, shift_vec, scale_vec):
    values = tok_rows.astype(F32)
    center = jnp.mean(values, axis=-1, keepdims=True)
    spread = jnp.mean(jnp.square(values - center), axis=-1, keepdims=True)
    scaled = (values - center) * lax.rsqrt(spread + EPSILON)
    return (scaled * (1.0 + scale_vec) + shift_vec).astype(BF)


def reduce_scatter_sp(parts):
    sp_count, n, c = parts.shape
    chips = sp_count // 2
    me = lax.axis_index("sp")
    core, chip = me % 2, me // 2
    pairs = parts.reshape(chips, 2, n, c)
    away = lax.dynamic_index_in_dim(pairs, 1 - core, 1, keepdims=False)
    got = lax.ppermute(away, "sp", [(i, i ^ 1) for i in range(sp_count)])
    mine = lax.dynamic_index_in_dim(pairs, core, 1, keepdims=False)
    both = (mine.astype(F32) + got.astype(F32)).astype(BF)
    total = lax.dynamic_index_in_dim(both, chip, 0, keepdims=False).astype(F32)
    for k in range(1, chips):
        piece = lax.dynamic_index_in_dim(both, (chip + k) % chips, 0, keepdims=False)
        perm = [(i, ((i // 2 + k) % chips) * 2 + i % 2) for i in range(sp_count)]
        total = total + lax.ppermute(piece, "sp", perm).astype(F32)
    return total


def all_gather_sp(piece):
    n, c = piece.shape
    sp_count = lax.axis_size("sp")
    chips = sp_count // 2
    me = lax.axis_index("sp")
    core, chip = me % 2, me // 2
    out = jnp.zeros((chips, 2, n, c), piece.dtype)
    for k in range(chips):
        got = piece
        if k:
            perm = [(i, ((i // 2 + k) % chips) * 2 + i % 2) for i in range(sp_count)]
            got = lax.ppermute(piece, "sp", perm)
        other = lax.ppermute(got, "sp", [(i, i ^ 1) for i in range(sp_count)])
        at = (chip - k) % chips
        out = lax.dynamic_update_slice(out, got[None, None], (at, core, 0, 0))
        out = lax.dynamic_update_slice(out, other[None, None], (at, 1 - core, 0, 0))
    return out.reshape(sp_count, n, c)


def attend(queries, key_rows, values, key_ok):
    factor = queries.shape[-1] ** (-0.5)
    scores = jnp.einsum("iqe,ike->iqk", queries, key_rows, preferred_element_type=F32) * factor
    scores = jnp.where(key_ok, scores, -jnp.inf)
    raw = jnp.exp(scores - jnp.max(scores, axis=-1, keepdims=True))
    att_weights = (raw / jnp.sum(raw, axis=-1, keepdims=True)).astype(BF)
    return jnp.einsum("iqk,ike->iqe", att_weights, values, preferred_element_type=F32).astype(BF)


def shards(tokens, modulation, w_qkv, w_out, w_up, w_down):
    frames, patches, width = tokens.shape
    sp_count, tp_count = lax.axis_size("sp"), lax.axis_size("tp")
    sp_me, tp_me = lax.axis_index("sp"), lax.axis_index("tp")
    heads = w_qkv.shape[2] // DH
    slab = width // sp_count
    groups = math.gcd(frames, tp_count)
    sub, f_own = tp_count // groups, frames // groups
    unit = 8 * sub
    padded = -(-patches // unit) * unit
    part = padded // sub
    rows = sub * sp_count * part
    own_rows = f_own * sp_count * part

    padded_tokens = jnp.pad(tokens, ((0, 0), (0, padded - patches), (0, 0)))
    mine = lax.dynamic_slice(
        padded_tokens, ((tp_me // sub) * f_own, (tp_me % sub) * part, 0), (f_own, part, width)
    )
    mod_mine = normalize(mine, modulation[0], modulation[1])
    both = jnp.stack([mod_mine, mine]).reshape(2, f_own, part, sp_count, slab)
    both = lax.all_to_all(both, "sp", split_axis=3, concat_axis=2, tiled=False)
    mod_slab = both[0].reshape(own_rows, slab)
    tok_slab = both[1].reshape(own_rows, slab)
    mod_a = spread_rows(mod_slab, frames, sub, f_own, rows)

    at = jnp.arange(rows)
    key_ok = ((at // (sp_count * part)) * part + at % part) < patches

    chunks = 2 if frames % (2 * sp_count) == 0 else 1
    f_chunk = frames // chunks
    f_split = math.gcd(f_chunk, sp_count)
    h_split = sp_count // f_split
    f_mine, h_mine = f_chunk // f_split, heads // h_split
    w_flat = w_qkv.reshape(slab, 3 * heads * DH)
    attn_parts = []
    for c in range(chunks):
        lhs = mod_a[c * f_chunk : (c + 1) * f_chunk].reshape(f_chunk * rows, slab)
        proj = jnp.dot(lhs, w_flat, preferred_element_type=F32).astype(BF)
        if h_split > 1:
            proj = proj.reshape(f_split, f_mine * rows, 3, h_split, h_mine * DH)
            proj = jnp.transpose(proj, (0, 3, 1, 2, 4))
        proj = proj.reshape(sp_count, f_mine * rows, 3 * h_mine * DH)
        proj = reduce_scatter_sp(proj).astype(BF).reshape(f_mine, rows, 3, h_mine, DH)
        proj = jnp.transpose(proj, (2, 0, 3, 1, 4)).reshape(3, f_mine * h_mine, rows, DH)
        att = attend(proj[0], proj[1], proj[2], key_ok)
        att = jnp.transpose(att.reshape(f_mine, h_mine, rows, DH), (0, 2, 1, 3))
        att = all_gather_sp(att.reshape(f_mine * rows, h_mine * DH))
        if h_split > 1:
            att = att.reshape(f_split, h_split, f_mine * rows, h_mine * DH)
            att = jnp.transpose(att, (0, 2, 1, 3))
        att = att.reshape(f_chunk * rows, heads * DH)
        attn_parts.append(jnp.dot(att, w_out, preferred_element_type=F32).astype(BF))
    attn_part = jnp.concatenate(attn_parts, 0).reshape(tp_count, own_rows, slab)
    attn_sum = lax.psum_scatter(attn_part, "tp", scatter_dimension=0, tiled=False).astype(F32)

    mod_slice = lax.dynamic_slice_in_dim(modulation, sp_me * slab, slab, 1)
    middle = (tok_slab.astype(F32) + mod_slice[2] * attn_sum).astype(BF)

    values = middle.astype(F32)
    mean_s = jnp.mean(values, axis=-1)
    dev_s = jnp.sum(jnp.square(values - mean_s[:, None]), axis=-1)
    stats = lax.all_gather(jnp.stack([mean_s, dev_s]), "sp", axis=0)
    center = jnp.mean(stats[:, 0], axis=0)
    spread = (jnp.sum(stats[:, 1], 0) + slab * jnp.sum(jnp.square(stats[:, 0] - center), 0)) / width
    scaled = (values - center[:, None]) * lax.rsqrt(spread + EPSILON)[:, None]
    mod_b = (scaled * (1.0 + mod_slice[4]) + mod_slice[3]).astype(BF)
    mod_b = spread_rows(mod_b, frames, sub, f_own, rows).reshape(frames * rows, slab)

    hid = w_up.shape[1] // MLP_CHUNKS
    share = frames * rows // sp_count
    acc = None
    for c in range(MLP_CHUNKS):
        up = jnp.dot(mod_b, w_up[:, c * hid : (c + 1) * hid], preferred_element_type=F32)
        up = reduce_scatter_sp(up.astype(BF).reshape(sp_count, share, hid))
        hidden = jax.nn.gelu(up, approximate=True).astype(BF)
        hidden = all_gather_sp(hidden).reshape(frames * rows, hid)
        term = jnp.dot(hidden, w_down[c * hid : (c + 1) * hid], preferred_element_type=F32)
        acc = term if acc is None else acc + term
    mlp_part = acc.astype(BF).reshape(tp_count, own_rows, slab)
    mlp_sum = lax.psum_scatter(mlp_part, "tp", scatter_dimension=0, tiled=False).astype(F32)
    block = (middle.astype(F32) + mod_slice[5] * mlp_sum).astype(BF)

    block = block.reshape(f_own, sp_count, part, slab)
    block = lax.all_to_all(block, "sp", split_axis=1, concat_axis=2, tiled=False)
    block = block.reshape(f_own, part, width)
    block = block.reshape(f_own, part, tp_count, width // tp_count)
    block = lax.all_to_all(block, "tp", split_axis=2, concat_axis=0, tiled=False)
    block = block.reshape(groups, sub, f_own, part, width // tp_count)
    block = jnp.transpose(block, (0, 2, 1, 3, 4)).reshape(frames, padded, width // tp_count)
    return block[:, :patches]


def spread_rows(own, frames, sub, f_own, rows):
    whole = lax.all_gather(own, "tp", axis=0, tiled=True)
    return whole.reshape(frames, rows, own.shape[1])


def solution(mesh):
    placed = (
        P(None, "sp", None),
        P(),
        P("sp", None, "tp"),
        P("tp", "sp"),
        P("sp", "tp"),
        P("tp", "sp"),
    )
    return jax.shard_map(
        shards, mesh=mesh, in_specs=placed, out_specs=P(None, "sp", "tp"), check_vma=False
    )
```

```python
import math

import jax
import jax.numpy as jnp
from jax import lax
from jax.sharding import PartitionSpec as P

DH = 128
EPSILON = 1e-06
MLP_CHUNKS = 4
BF = jnp.bfloat16
F32 = jnp.float32


def normalize(tok_rows, shift_vec, scale_vec):
    values = tok_rows.astype(F32)
    center = jnp.mean(values, axis=-1, keepdims=True)
    spread = jnp.mean(jnp.square(values - center), axis=-1, keepdims=True)
    scaled = (values - center) * lax.rsqrt(spread + EPSILON)
    return (scaled * (1.0 + scale_vec) + shift_vec).astype(BF)


def reduce_scatter_sp(parts):
    sp_count, n, c = parts.shape
    chips = sp_count // 2
    me = lax.axis_index("sp")
    core, chip = me % 2, me // 2
    pairs = parts.reshape(chips, 2, n, c)
    away = lax.dynamic_index_in_dim(pairs, 1 - core, 1, keepdims=False)
    got = lax.ppermute(away, "sp", [(i, i ^ 1) for i in range(sp_count)])
    mine = lax.dynamic_index_in_dim(pairs, core, 1, keepdims=False)
    both = (mine.astype(F32) + got.astype(F32)).astype(BF)
    total = lax.dynamic_index_in_dim(both, chip, 0, keepdims=False).astype(F32)
    for k in range(1, chips):
        piece = lax.dynamic_index_in_dim(both, (chip + k) % chips, 0, keepdims=False)
        perm = [(i, ((i // 2 + k) % chips) * 2 + i % 2) for i in range(sp_count)]
        total = total + lax.ppermute(piece, "sp", perm).astype(F32)
    return total


def all_gather_sp(piece):
    n, c = piece.shape
    sp_count = lax.axis_size("sp")
    chips = sp_count // 2
    me = lax.axis_index("sp")
    core, chip = me % 2, me // 2
    out = jnp.zeros((chips, 2, n, c), piece.dtype)
    for k in range(chips):
        got = piece
        if k:
            perm = [(i, ((i // 2 + k) % chips) * 2 + i % 2) for i in range(sp_count)]
            got = lax.ppermute(piece, "sp", perm)
        other = lax.ppermute(got, "sp", [(i, i ^ 1) for i in range(sp_count)])
        at = (chip - k) % chips
        out = lax.dynamic_update_slice(out, got[None, None], (at, core, 0, 0))
        out = lax.dynamic_update_slice(out, other[None, None], (at, 1 - core, 0, 0))
    return out.reshape(sp_count, n, c)


def attend(queries, key_rows, values, key_ok):
    factor = queries.shape[-1] ** (-0.5)
    scores = jnp.einsum("iqe,ike->iqk", queries, key_rows, preferred_element_type=F32) * factor
    scores = jnp.where(key_ok, scores, -jnp.inf)
    raw = jnp.exp(scores - jnp.max(scores, axis=-1, keepdims=True))
    att_weights = (raw / jnp.sum(raw, axis=-1, keepdims=True)).astype(BF)
    return jnp.einsum("iqk,ike->iqe", att_weights, values, preferred_element_type=F32).astype(BF)


def shards(tokens, modulation, w_qkv, w_out, w_up, w_down):
    frames, patches, width = tokens.shape
    sp_count, tp_count = lax.axis_size("sp"), lax.axis_size("tp")
    sp_me, tp_me = lax.axis_index("sp"), lax.axis_index("tp")
    heads = w_qkv.shape[2] // DH
    slab = width // sp_count
    groups = math.gcd(frames, tp_count)
    sub, f_own = tp_count // groups, frames // groups
    unit = 8 * sub
    padded = -(-patches // unit) * unit
    part = padded // sub
    rows = sub * sp_count * part
    own_rows = f_own * sp_count * part

    padded_tokens = jnp.pad(tokens, ((0, 0), (0, padded - patches), (0, 0)))
    mine = lax.dynamic_slice(
        padded_tokens, ((tp_me // sub) * f_own, (tp_me % sub) * part, 0), (f_own, part, width)
    )
    mod_mine = normalize(mine, modulation[0], modulation[1])
    def to_slabs(value):
        value = value.reshape(f_own * part, sp_count, slab)
        value = exchange(jnp.transpose(value, (1, 0, 2)), "sp")
        value = value.reshape(sp_count, f_own, part, slab)
        return jnp.transpose(value, (1, 0, 2, 3)).reshape(own_rows, slab)

    mod_slab, tok_slab = to_slabs(mod_mine), to_slabs(mine)
    mod_a = spread_rows(mod_slab, frames, sub, f_own, rows)

    at = jnp.arange(rows)
    key_ok = ((at // (sp_count * part)) * part + at % part) < patches

    chunks = 2 if frames % (2 * sp_count) == 0 else 1
    f_chunk = frames // chunks
    f_split = math.gcd(f_chunk, sp_count)
    h_split = sp_count // f_split
    f_mine, h_mine = f_chunk // f_split, heads // h_split
    w_flat = w_qkv.reshape(slab, 3 * heads * DH)
    attn_parts = []
    for c in range(chunks):
        lhs = mod_a[c * f_chunk : (c + 1) * f_chunk].reshape(f_chunk * rows, slab)
        proj = jnp.dot(lhs, w_flat, preferred_element_type=F32).astype(BF)
        if h_split > 1:
            proj = proj.reshape(f_split, f_mine * rows, 3, h_split, h_mine * DH)
            proj = jnp.transpose(proj, (0, 3, 1, 2, 4))
        proj = proj.reshape(sp_count, f_mine * rows, 3 * h_mine * DH)
        proj = reduce_scatter_sp(proj).astype(BF).reshape(f_mine, rows, 3, h_mine, DH)
        proj = jnp.transpose(proj, (2, 0, 3, 1, 4)).reshape(3, f_mine * h_mine, rows, DH)
        att = attend(proj[0], proj[1], proj[2], key_ok)
        att = jnp.transpose(att.reshape(f_mine, h_mine, rows, DH), (0, 2, 1, 3))
        att = all_gather_sp(att.reshape(f_mine * rows, h_mine * DH))
        if h_split > 1:
            att = att.reshape(f_split, h_split, f_mine * rows, h_mine * DH)
            att = jnp.transpose(att, (0, 2, 1, 3))
        att = att.reshape(f_chunk * rows, heads * DH)
        attn_parts.append(jnp.dot(att, w_out, preferred_element_type=F32).astype(BF))
    attn_part = jnp.concatenate(attn_parts, 0).reshape(tp_count, own_rows, slab)
    attn_sum = reduce_scatter_tp(attn_part)

    mod_slice = lax.dynamic_slice_in_dim(modulation, sp_me * slab, slab, 1)
    middle = (tok_slab.astype(F32) + mod_slice[2] * attn_sum).astype(BF)

    values = middle.astype(F32)
    mean_s = jnp.mean(values, axis=-1)
    dev_s = jnp.sum(jnp.square(values - mean_s[:, None]), axis=-1)
    stats = lax.all_gather(jnp.stack([mean_s, dev_s]), "sp", axis=0)
    center = jnp.mean(stats[:, 0], axis=0)
    spread = (jnp.sum(stats[:, 1], 0) + slab * jnp.sum(jnp.square(stats[:, 0] - center), 0)) / width
    scaled = (values - center[:, None]) * lax.rsqrt(spread + EPSILON)[:, None]
    mod_b = (scaled * (1.0 + mod_slice[4]) + mod_slice[3]).astype(BF)
    mod_b = spread_rows(mod_b, frames, sub, f_own, rows).reshape(frames * rows, slab)

    hid = w_up.shape[1] // MLP_CHUNKS
    share = frames * rows // sp_count
    acc = None
    for c in range(MLP_CHUNKS):
        up = jnp.dot(mod_b, w_up[:, c * hid : (c + 1) * hid], preferred_element_type=F32)
        up = reduce_scatter_sp(up.astype(BF).reshape(sp_count, share, hid))
        hidden = jax.nn.gelu(up, approximate=True).astype(BF)
        hidden = all_gather_sp(hidden).reshape(frames * rows, hid)
        term = jnp.dot(hidden, w_down[c * hid : (c + 1) * hid], preferred_element_type=F32)
        acc = term if acc is None else acc + term
    mlp_part = acc.astype(BF).reshape(tp_count, own_rows, slab)
    mlp_sum = reduce_scatter_tp(mlp_part)
    block = (middle.astype(F32) + mod_slice[5] * mlp_sum).astype(BF)

    block = jnp.transpose(block.reshape(f_own, sp_count, part, slab), (1, 0, 2, 3))
    block = exchange(block.reshape(sp_count, f_own * part, slab), "sp")
    block = jnp.transpose(block, (1, 0, 2)).reshape(f_own * part, tp_count, width // tp_count)
    block = exchange(jnp.transpose(block, (1, 0, 2)), "tp")
    block = block.reshape(groups, sub, f_own, part, width // tp_count)
    block = jnp.transpose(block, (0, 2, 1, 3, 4)).reshape(frames, padded, width // tp_count)
    return block[:, :patches]


def tp_grid():
    count = lax.axis_size("tp")
    lanes = 2 ** ((count.bit_length() - 1) // 2)
    return count, count // lanes, lanes


def ring_shift(value, k):
    count, ring, lanes = tp_grid()
    return lax.ppermute(
        value, "tp", [(i, ((i // lanes + k) % ring) * lanes + i % lanes) for i in range(count)]
    )


def lane_shift(value, k):
    count, ring, lanes = tp_grid()
    return lax.ppermute(
        value, "tp", [(i, (i // lanes) * lanes + (i + k) % lanes) for i in range(count)]
    )


def ring_pieces(piece):
    ring = tp_grid()[1]
    if ring != 4:
        return [(k, ring_shift(piece, k) if k else piece) for k in range(ring)]
    half = piece.shape[1] // 2
    left, right = ring_shift(piece, 1), ring_shift(piece, -1)
    far = [ring_shift(left[:, :half], 1), ring_shift(right[:, half:], -1)]
    return [(0, piece), (1, left), (3, right), (2, jnp.concatenate(far, 1))]


def ring_reduce(parts):
    ring = parts.shape[0]
    _, _, lanes = tp_grid()
    place = lax.axis_index("tp") // lanes

    def part(k):
        return lax.dynamic_index_in_dim(parts, (place + k) % ring, 0, keepdims=False)

    total = part(0).astype(F32)
    if ring != 4:
        for k in range(1, ring):
            total = total + ring_shift(part(k), k).astype(F32)
        return total
    half = parts.shape[2] // 2
    far = part(2)
    from_left, from_right = ring_shift(far[:, :half], 1), ring_shift(far[:, half:], -1)
    ahead, behind = part(1), part(3)
    low = (ahead[:, :half].astype(F32) + from_left.astype(F32)).astype(BF)
    high = (behind[:, half:].astype(F32) + from_right.astype(F32)).astype(BF)
    ahead = jnp.concatenate([low, ahead[:, half:]], 1)
    behind = jnp.concatenate([behind[:, :half], high], 1)
    return total + ring_shift(ahead, 1).astype(F32) + ring_shift(behind, -1).astype(F32)


def reduce_scatter_tp(parts):
    count, ring, lanes = tp_grid()
    lane = lax.axis_index("tp") % lanes
    grid = parts.reshape((ring, lanes) + parts.shape[1:])
    total = None
    for k in list(range(1, lanes)) + [0]:
        picked = lax.dynamic_index_in_dim(grid, (lane + k) % lanes, 1, keepdims=False)
        summed = ring_reduce(picked)
        if k:
            summed = lane_shift(summed.astype(BF), k).astype(F32)
        total = summed if total is None else total + summed
    return total


def spread_rows(own, frames, sub, f_own, rows):
    count, ring, lanes = tp_grid()
    me = lax.axis_index("tp")
    place, lane = me // lanes, me % lanes
    out = jnp.zeros((count,) + own.shape, own.dtype)
    for k in range(lanes):
        column = lane_shift(own, k) if k else own
        for back, piece in ring_pieces(column):
            at = ((place - back) % ring) * lanes + (lane - k) % lanes
            out = lax.dynamic_update_slice(out, piece[None], (at, 0, 0))
    return out.reshape(frames, rows, own.shape[1])


def exchange(parts, axis):
    count = parts.shape[0]
    me = lax.axis_index(axis)
    out = parts
    for k in range(1, count):
        piece = lax.dynamic_index_in_dim(parts, (me + k) % count, 0)
        got = lax.ppermute(piece, axis, [(i, (i + k) % count) for i in range(count)])
        out = lax.dynamic_update_slice_in_dim(out, got, (me - k) % count, 0)
    return out


def solution(mesh):
    placed = (
        P(None, "sp", None),
        P(),
        P("sp", None, "tp"),
        P("tp", "sp"),
        P("sp", "tp"),
        P("tp", "sp"),
    )
    return jax.shard_map(
        shards, mesh=mesh, in_specs=placed, out_specs=P(None, "sp", "tp"), check_vma=False
    )
```
